32 devices in a mesh: rep: 4 (over z), gy: 2 (over y), gz: 4 (over x, core).
Axes of the slice: x: 2, y: 2, z: 4, core: 2. Of those that a mesh axis runs over, the one named last changes fastest.
Arguments:
- charges: float32 [1024, 256, 128], P(('rep', 'gz'), 'gy'), may hold values from -6 to 6
- green: float32 [256, 256, 128], P('rep', ('gy', 'gz')), may hold values from 0.1 to 3
Outputs:
- potential: float32 [1024, 256, 128], P(('rep', 'gz'), 'gy')
The draws below stay inside these ranges and needn't reach their ends.
All inputs are finite; a program needn't handle non-finite values.
Results may differ from the reference program's by a relative error of at most 0.00007.
Values sent between devices are 32-bit elements; how exact they have to be, the bound alone decides.
A program may use at most 64 MiB of HBM per device.

```python
import math
import jax
import jax.numpy as jnp
from jax import lax

NG = 256
NZ = 128
REPLICAS = 4


def levels(key, dims, shards, low, top_value):
    gain = 1.0
    for axis_at, blocks in shards:
        steps = jax.random.uniform(jax.random.fold_in(jax.random.fold_in(key, 6), axis_at), (blocks,), jnp.float32, low / len(shards), top_value / len(shards))
        gain = gain * jnp.repeat(jnp.exp(steps), dims[axis_at] // blocks).reshape((-1,) + (1,) * (len(dims) - 1 - axis_at))
    return gain


def bell_draw(stream_key, shape, scale, reach, split=(), kind=jnp.bfloat16):
    array = scale * jax.random.normal(stream_key, shape, jnp.float32)
    if split:
        array = array * levels(stream_key, shape, split, -0.22, 0.18)
    return jnp.clip(array, -reach, reach).astype(kind)


def setup_inputs(seed: int = 0) -> dict:
    streams_of = jax.random.split(jax.random.key(seed), 3)
    return {
        "charges": bell_draw(streams_of[0], (REPLICAS * NG, NG, NZ), 1.0, 6.0, ((0, 16), (1, 2)), jnp.float32),
        "green": jnp.clip(jnp.exp(math.log(3.0) - 3.4011974 * jax.random.uniform(streams_of[1], (NG, NG, NZ), jnp.float32) ** levels(streams_of[1], (NG, NG, NZ), ((0, 4), (1, 8)), -0.2, 0.2)), 0.1, 3.0),
    }


def reference(charges, green):
    stacked = charges.reshape(REPLICAS, NG, NG, NZ)

    def single(charge):
        spectrum = jnp.fft.fftn(charge) * green
        return jnp.real(jnp.fft.ifftn(spectrum)).astype(jnp.float32)

    return lax.map(single, stacked).reshape(REPLICAS * NG, NG, NZ)
```

```python
import functools
import math

import jax
import jax.numpy as jnp
import numpy as np
from jax import lax
from jax.experimental import pallas as pl
from jax.experimental.pallas import tpu as pltpu
from jax.sharding import PartitionSpec as P

NG = 256
NZ = 128


two_pi = 2.0 * math.pi
highest = lax.Precision.HIGHEST


def tables(length, rows_index, cols_index):
    phase = rows_index[:, None] * cols_index[None, :] % length
    angle = phase.astype(jnp.float32) * (two_pi / length)
    return (jnp.cos(angle), jnp.sin(angle))


def reflect(values):
    return jnp.roll(jnp.flip(values, (1, 2)), (1, 1), axis=(1, 2))


def slab_plan(charges, green):
    gy_count = lax.axis_size("gy")
    gz_count = lax.axis_size("gz")
    groups = gy_count * gz_count
    half = NZ // 2
    per_device = half // groups
    col_block = charges.shape[1]
    depth = jnp.arange(NZ, dtype=jnp.int32)
    bins = jnp.arange(half, dtype=jnp.int32)
    indices = jnp.arange(NG, dtype=jnp.int32)
    cos_depth, sin_depth = tables(NZ, depth, bins)
    alternate = (1 - 2 * (depth % 2)).astype(jnp.float32)
    sin_packed = jnp.where(bins[None, :] == 0, -alternate[:, None], sin_depth)
    spec_re = jnp.einsum("xyz,zk->kxy", charges, cos_depth, precision=highest)
    spec_im = -jnp.einsum("xyz,zk->kxy", charges, sin_packed, precision=highest)
    own = jnp.moveaxis(green[:, :, :half], 2, 0)
    mirror = jnp.concatenate(
        [green[:, :, half : half + 1], jnp.flip(green[:, :, half + 1 :], 2)], axis=2
    )
    mirror = jnp.moveaxis(mirror, 2, 0)
    own, mirror = (
        lax.all_to_all(own, ("gy", "gz"), split_axis=0, concat_axis=2, tiled=True),
        lax.all_to_all(mirror, ("gy", "gz"), split_axis=0, concat_axis=2, tiled=True),
    )
    own, mirror = (
        lax.all_gather(own, "rep", axis=1, tiled=True),
        lax.all_gather(mirror, "rep", axis=1, tiled=True),
    )
    plane_re, plane_im = (
        lax.all_to_all(spec_re, ("gy", "gz"), split_axis=0, concat_axis=1, tiled=True),
        lax.all_to_all(spec_im, ("gy", "gz"), split_axis=0, concat_axis=1, tiled=True),
    )
    plane_re = plane_re.reshape(per_device, gy_count, NG, col_block)
    plane_im = plane_im.reshape(per_device, gy_count, NG, col_block)
    cos_plain, sin_plain = tables(NG, indices, indices)
    wide_cos = cos_plain.reshape(NG, gy_count, col_block)
    wide_sin = sin_plain.reshape(NG, gy_count, col_block)

    def second_in(matrix, values):
        return jnp.einsum("kgc,bgxc->bxk", matrix, values, precision=highest)

    def first_in(matrix, values):
        return jnp.einsum("kx,bxj->bkj", matrix, values, precision=highest)

    inner_re = second_in(wide_cos, plane_re) + second_in(wide_sin, plane_im)
    inner_im = second_in(wide_cos, plane_im) - second_in(wide_sin, plane_re)
    freq_re = first_in(cos_plain, inner_re) + first_in(sin_plain, inner_im)
    freq_im = first_in(cos_plain, inner_im) - first_in(sin_plain, inner_re)
    slot = lax.axis_index("gy") * gz_count + lax.axis_index("gz")
    packed = ((slot == 0) & (jnp.arange(per_device) == 0))[:, None, None]
    plain_gain = 0.5 * (own + reflect(mirror))
    first_gain = jnp.where(packed, 0.5 * (own + reflect(own)), plain_gain)
    second_gain = jnp.where(packed, 0.5 * (mirror + reflect(mirror)), plain_gain)
    mean_gain = 0.5 * (first_gain + second_gain)
    odd_gain = 0.5 * (first_gain - second_gain)
    prod_re = freq_re * mean_gain + reflect(freq_re) * odd_gain
    prod_im = freq_im * mean_gain - reflect(freq_im) * odd_gain
    undo_re = first_in(cos_plain, prod_re) - first_in(sin_plain, prod_im)
    undo_im = first_in(sin_plain, prod_re) + first_in(cos_plain, prod_im)

    def second_out(matrix, values):
        return jnp.einsum("kgc,bxk->bgxc", matrix, values, precision=highest)

    cells_re = second_out(wide_cos, undo_re) - second_out(wide_sin, undo_im)
    cells_im = second_out(wide_sin, undo_re) + second_out(wide_cos, undo_im)
    cells_re = cells_re.reshape(per_device, gy_count * NG, col_block)
    cells_im = cells_im.reshape(per_device, gy_count * NG, col_block)
    home_re, home_im = (
        lax.all_to_all(cells_re, ("gy", "gz"), split_axis=1, concat_axis=0, tiled=True),
        lax.all_to_all(cells_im, ("gy", "gz"), split_axis=1, concat_axis=0, tiled=True),
    )
    weight = jnp.where(bins == 0, 1.0, 2.0).astype(jnp.float32)
    cos_back = (cos_depth * weight[None, :]).T
    sin_back = jnp.where(bins[:, None] == 0, alternate[None, :], -2.0 * sin_depth.T)
    result_field = jnp.einsum("kxy,kz->xyz", home_re, cos_back, precision=highest)
    result_field = result_field + jnp.einsum("kxy,kz->xyz", home_im, sin_back, precision=highest)
    return result_field / (NG * NG * NZ)


f32 = jnp.float32
bf16 = jnp.bfloat16
MESH = pl.DeviceIdType.MESH
PARTS = 2


def split(values):
    high = values.astype(bf16)
    return high, (values - high.astype(f32)).astype(bf16)


def split_table(table):
    rounded = table.astype(jnp.bfloat16)
    high = jnp.asarray(rounded)
    low = jnp.asarray((table - rounded.astype(np.float64)).astype(jnp.bfloat16))
    return high, low


def dot(left, right, dims=((1,), (0,))):
    return lax.dot_general(left, right, (dims, ((), ())), preferred_element_type=f32)


def dot_table(values, table_high, table_low, dims=((1,), (0,))):
    high, low = split(values)
    return dot(high, table_high, dims) + (dot(low, table_high, dims) + dot(high, table_low, dims))


def table_dot(table_high, table_low, values, dims=((1,), (0,))):
    high, low = split(values)
    return dot(table_high, high, dims) + (dot(table_high, low, dims) + dot(table_low, high, dims))


def depth_tables(length, groups, bins_each):
    per_part = bins_each // PARTS
    forward, back = [], []
    z = np.arange(length)
    alternate = 1.0 - 2.0 * (z % 2)
    for start in range(0, groups * bins_each, per_part):
        for imaginary in (False, True):
            for k in range(start, start + per_part):
                angle = 2.0 * np.pi * ((k * z) % length) / length
                if k == 0:
                    forward.append(alternate if imaginary else np.ones(length))
                    back.append(alternate if imaginary else np.ones(length))
                else:
                    forward.append(-np.sin(angle) if imaginary else np.cos(angle))
                    back.append(-2.0 * np.sin(angle) if imaginary else 2.0 * np.cos(angle))
    return np.stack(forward), np.stack(back)


def depth_in_kernel(high_ref, low_ref, cells_ref, out_ref):
    rows, cols, depth = cells_ref.shape
    groups, parts, _, _ = out_ref.shape
    values = cells_ref[...].reshape(rows * cols, depth)
    result = table_dot(high_ref[...], low_ref[...], values, ((1,), (1,)))
    for row in range(rows):
        piece = result[:, row * cols : (row + 1) * cols]
        out_ref[:, :, row * 8 : (row + 1) * 8, :] = piece.reshape(groups, parts, 8, cols)


def depth_out_kernel(high_ref, low_ref, spec_ref, out_ref):
    rows, cols, depth = out_ref.shape
    pieces = [
        spec_ref[:, :, row * 8 : (row + 1) * 8, :].reshape(high_ref.shape[0], cols) for row in range(rows)
    ]
    values = jnp.concatenate(pieces, axis=1)
    result = dot_table(values, high_ref[...], low_ref[...], ((0,), (0,)))
    out_ref[...] = result.reshape(rows, cols, depth)


def planes_kernel(
    gy_count, gz_count, reps,
    spec_ref, gains_ref, mat_h, mat_l, tra_h, tra_l, flip_ref, home_ref,
    planes, green, freq,
    fwd_send, fwd_recv, back_send, back_recv, green_send, green_recv, right_send, left_send, line_recv, own_sem,
):
    groups = gy_count * gz_count
    rep, gy, gz = lax.axis_index("rep"), lax.axis_index("gy"), lax.axis_index("gz")
    slot = gy * gz_count + gz
    rows = spec_ref.shape[2] // 8
    ng = flip_ref.shape[0]
    piece = gains_ref.shape[1]

    def partner(step):
        there_y = lax.rem(gy + step // gz_count, gy_count)
        there_z = lax.rem(gz + step % gz_count, gz_count)
        return there_y * gz_count + there_z, {"rep": rep, "gy": there_y, "gz": there_z}

    def along(step):
        return {"rep": lax.rem(rep + step + reps, reps), "gy": gy, "gz": gz}

    order = sorted(range(1, groups), key=lambda s: (-(s % gz_count), s))

    barrier = pltpu.get_barrier_semaphore()
    for step in order:
        pl.semaphore_signal(barrier, inc=1, device_id=partner(step)[1], device_id_type=MESH)
    for step in (1, -1):
        pl.semaphore_signal(barrier, inc=1, device_id=along(step), device_id_type=MESH)
    pl.semaphore_wait(barrier, groups + 1)

    def green_copy(step, source):
        there, device = partner(step)
        return pltpu.make_async_remote_copy(
            src_ref=gains_ref.at[there], dst_ref=green.at[rep, pl.ds(source * piece, piece), :],
            send_sem=green_send.at[there], recv_sem=green_recv.at[source], device_id=device, device_id_type=MESH)

    def fwd_copy(step, source, part):
        there, device = partner(step)
        return pltpu.make_async_remote_copy(
            src_ref=spec_ref.at[there, part], dst_ref=planes.at[source, part],
            send_sem=fwd_send.at[there, part], recv_sem=fwd_recv.at[source, part], device_id=device, device_id_type=MESH)

    def back_copy(step, source, part):
        there, device = partner(step)
        return pltpu.make_async_remote_copy(
            src_ref=planes.at[there, part], dst_ref=home_ref.at[source, part],
            send_sem=back_send.at[there, part], recv_sem=back_recv.at[source, part], device_id=device, device_id_type=MESH)

    def line_copy(block, sem, step):
        return pltpu.make_async_remote_copy(
            src_ref=green.at[block], dst_ref=green.at[block], send_sem=sem, recv_sem=line_recv.at[block],
            device_id=along(step), device_id_type=MESH)

    for step in order:
        green_copy(step, slot).start()
    own_green = pltpu.make_async_copy(gains_ref.at[slot], green.at[rep, pl.ds(slot * piece, piece), :], own_sem.at[0])
    own_green.start()
    own_planes = [pltpu.make_async_copy(spec_ref.at[slot, h], planes.at[slot, h], own_sem.at[1 + h]) for h in range(PARTS)]
    for copy in own_planes:
        copy.start()
    own_green.wait()
    for step in order:
        green_copy(step, partner(step)[0]).wait_recv()

    @pl.when(rep + 1 < reps)
    def _():
        line_copy(rep, right_send.at[0], 1).start()

    @pl.when(rep >= 1)
    def _():
        line_copy(rep, left_send.at[0], -1).start()

    for part in range(PARTS):
        for step in order:
            fwd_copy(step, slot, part).start()

    def relay(hop):
        @pl.when(rep >= hop)
        def _():
            line_copy(rep - hop, right_send.at[hop], 1).wait_recv()

        @pl.when((rep >= hop) & (rep + 1 < reps))
        def _():
            line_copy(rep - hop, right_send.at[hop], 1).start()

        @pl.when(rep + hop < reps)
        def _():
            line_copy(rep + hop, left_send.at[hop], -1).wait_recv()

        @pl.when((rep + hop < reps) & (rep >= 1))
        def _():
            line_copy(rep + hop, left_send.at[hop], -1).start()

    def load_plane(part, row):
        bands = []
        for y in range(gy_count):
            bands.append(jnp.concatenate(
                [planes[y * gz_count + x, part, pl.ds(row, rows, stride=8), :] for x in range(gz_count)], axis=0))
        return jnp.concatenate(bands, axis=1)

    def forward(part):
        def body(p, carry):
            values = jnp.concatenate([load_plane(part, p), load_plane(part, 4 + p)], axis=1)
            inner = dot_table(values, mat_h[...], mat_l[...])
            inner = jnp.concatenate([inner[:, :ng], inner[:, ng:]], axis=0)
            freq[part * 4 + p] = table_dot(tra_h[...], tra_l[...], inner)
            return carry

        lax.fori_loop(0, 4, body, 0)

    def reflect_plane(values):
        flip = flip_ref[...]
        high, low = split(values)
        turned = dot(flip, high) + dot(flip, low)
        high, low = split(turned)
        return dot(high, flip) + dot(low, flip)

    def backward(part):
        def body(p, carry):
            plane = part * 4 + p
            own, mirror = [], []
            lane = lax.broadcasted_iota(jnp.int32, (ng, 128), 1)
            for r in range(0, reps, 2):
                one = green[r, pl.ds(plane, ng, stride=8), :]
                two = green[r + 1, pl.ds(plane, ng, stride=8), :]
                own.append(jnp.where(lane < 64, one, pltpu.roll(two, 64, 1)))
                mirror.append(jnp.where(lane < 64, pltpu.roll(one, 64, 1), two))
            own = jnp.concatenate(own, axis=1).T
            mirror = jnp.concatenate(mirror, axis=1).T
            packed = (slot == 0) & (plane == 0)

            @pl.when(jnp.logical_not(packed))
            def _():
                gain = 0.5 * (own + reflect_plane(mirror))
                freq[plane] = freq[plane] * jnp.concatenate([gain, gain], axis=0)

            @pl.when(packed)
            def _():
                first = 0.5 * (own + reflect_plane(own))
                second = 0.5 * (mirror + reflect_plane(mirror))
                mean, odd = 0.5 * (first + second), 0.5 * (first - second)
                real, imag = freq[plane, :ng, :], freq[plane, ng:, :]
                freq[plane, :ng, :] = real * mean + reflect_plane(real) * odd
                freq[plane, ng:, :] = imag * mean - reflect_plane(imag) * odd

            undo = table_dot(mat_h[...], mat_l[...], freq[plane])
            undo = jnp.concatenate([undo[:ng], undo[ng:]], axis=1)
            cells = dot_table(undo, tra_h[...], tra_l[...])
            cols = ng // gy_count
            for c in range(2):
                for y in range(gy_count):
                    for x in range(gz_count):
                        planes[y * gz_count + x, part, pl.ds(c * 4 + p, rows, stride=8), :] = cells[
                            x * rows : (x + 1) * rows, c * ng + y * cols : c * ng + (y + 1) * cols]
            return carry

        lax.fori_loop(0, 4, body, 0)

    for part in range(PARTS):
        own_planes[part].wait()
        for step in order:
            fwd_copy(step, partner(step)[0], part).wait_recv()
        forward(part)
        relay(part + 1)
    for hop in range(PARTS + 1, reps):
        relay(hop)

    own_home = [pltpu.make_async_copy(planes.at[slot, h], home_ref.at[slot, h], own_sem.at[1 + h]) for h in range(PARTS)]
    for part in range(PARTS):
        backward(part)
        for step in order:
            back_copy(step, slot, part).start()
        own_home[part].start()
    for step in order:
        green_copy(step, slot).wait_send()
    for part in range(PARTS):
        for step in order:
            fwd_copy(step, slot, part).wait_send()
    for hop in range(reps):
        @pl.when((rep >= hop) & (rep + 1 < reps))
        def _():
            line_copy(rep - hop, right_send.at[hop], 1).wait_send()

        @pl.when((rep + hop < reps) & (rep >= 1))
        def _():
            line_copy(rep + hop, left_send.at[hop], -1).wait_send()
    for part in range(PARTS):
        own_home[part].wait()
        for step in order:
            back_copy(step, slot, part).wait_send()
            back_copy(step, partner(step)[0], part).wait_recv()


def fused_plan(charges, green):
    gy_count, gz_count, reps = lax.axis_size("gy"), lax.axis_size("gz"), lax.axis_size("rep")
    groups = gy_count * gz_count
    rows, cols, depth = charges.shape
    ng = rows * gz_count
    half = depth // 2
    each = half // groups
    step = 8
    forward_table, back_table = depth_tables(depth, groups, each)
    fwd_h, fwd_l = split_table(forward_table)
    back_h, back_l = split_table(back_table / (ng * ng * depth))
    vmem = pl.BlockSpec(memory_space=pltpu.VMEM)
    table_spec = pl.BlockSpec((depth, depth), lambda i: (0, 0))
    cells_spec = pl.BlockSpec((step, cols, depth), lambda i: (i, 0, 0))
    spec_spec = pl.BlockSpec((groups, PARTS, step * 8, cols), lambda i: (0, 0, i, 0))
    spec_shape = jax.ShapeDtypeStruct((groups, PARTS, rows * 8, cols), f32)
    limit = pltpu.CompilerParams(vmem_limit_bytes=40 * 2**20)
    spec = pl.pallas_call(
        depth_in_kernel, grid=(rows // step,), out_shape=spec_shape, name="depth_in",
        in_specs=[table_spec, table_spec, cells_spec], out_specs=spec_spec, compiler_params=limit,
    )(fwd_h, fwd_l, charges)

    k1, k2, _ = green.shape
    own_index = np.arange(half)
    opposite = np.where(own_index == 0, half, depth - own_index)
    pick = np.zeros((2, half, depth), np.float32)
    pick[0, own_index, own_index] = 1.0
    pick[1, own_index, opposite] = 1.0
    gains = jnp.einsum("mqz,xyz->yqmx", jnp.asarray(pick), green, precision=lax.Precision.HIGHEST)
    gains = gains.reshape(k2, groups, each, 2 * k1).transpose(1, 0, 2, 3).reshape(groups, k2 * each, 2 * k1)

    index = np.arange(ng)
    angle = 2.0 * np.pi * ((index[:, None] * index[None, :]) % ng) / ng
    cos, sin = np.cos(angle), np.sin(angle)
    matrix = np.block([[cos, -sin], [sin, cos]])
    mat_h, mat_l = split_table(matrix)
    tra_h, tra_l = split_table(np.ascontiguousarray(matrix.T))
    flip = jnp.asarray((index[:, None] + index[None, :]) % ng == 0, bf16)

    dma = pltpu.SemaphoreType.DMA
    home = pl.pallas_call(
        functools.partial(planes_kernel, gy_count, gz_count, reps),
        out_shape=spec_shape, name="planes",
        in_specs=[vmem] * 7, out_specs=pl.BlockSpec(memory_space=pl.ANY),
        scratch_shapes=[
            pltpu.VMEM(spec_shape.shape, f32),
            pltpu.VMEM((reps, ng * each, 2 * k1), f32),
            pltpu.VMEM((each, 2 * ng, ng), f32),
            dma((groups, PARTS)), dma((groups, PARTS)), dma((groups, PARTS)), dma((groups, PARTS)),
            dma((groups,)), dma((groups,)), dma((reps,)), dma((reps,)), dma((reps,)), dma((1 + PARTS,)),
        ],
        compiler_params=pltpu.CompilerParams(
            collective_id=0, has_side_effects=True, vmem_limit_bytes=58 * 2**20),
    )(spec, gains, mat_h, mat_l, tra_h, tra_l, flip)

    return pl.pallas_call(
        depth_out_kernel, grid=(rows // step,), out_shape=jax.ShapeDtypeStruct(charges.shape, f32), name="depth_out",
        in_specs=[table_spec, table_spec, spec_spec], out_specs=cells_spec, compiler_params=limit,
    )(back_h, back_l, home)


def on_device(charges, green):
    groups = lax.axis_size("gy") * lax.axis_size("gz")
    rows, cols, depth = charges.shape
    aligned = (
        cols % 128 == 0 and depth % 128 == 0 and depth == 16 * groups and rows % 8 == 0
        and green.shape[0] == 64 and lax.axis_size("rep") % 2 == 0 and lax.axis_size("rep") > 2
        and rows * lax.axis_size("gz") == cols * lax.axis_size("gy")
    )
    return fused_plan(charges, green) if aligned else slab_plan(charges, green)


def solution(mesh):
    placed = (P(("rep", "gz"), "gy", None), P("rep", ("gy", "gz"), None))
    return jax.shard_map(
        on_device,
        mesh=mesh,
        in_specs=placed,
        out_specs=P(("rep", "gz"), "gy", None),
        check_vma=False,
    )
```

```python
import functools
import math

import jax
import jax.numpy as jnp
import numpy as np
from jax import lax
from jax.experimental import pallas as pl
from jax.experimental.pallas import tpu as pltpu
from jax.sharding import PartitionSpec as P

NG = 256
NZ = 128


two_pi = 2.0 * math.pi
highest = lax.Precision.HIGHEST


def tables(length, rows_index, cols_index):
    phase = rows_index[:, None] * cols_index[None, :] % length
    angle = phase.astype(jnp.float32) * (two_pi / length)
    return (jnp.cos(angle), jnp.sin(angle))


def reflect(values):
    return jnp.roll(jnp.flip(values, (1, 2)), (1, 1), axis=(1, 2))


def slab_plan(charges, green):
    gy_count = lax.axis_size("gy")
    gz_count = lax.axis_size("gz")
    groups = gy_count * gz_count
    half = NZ // 2
    per_device = half // groups
    col_block = charges.shape[1]
    depth = jnp.arange(NZ, dtype=jnp.int32)
    bins = jnp.arange(half, dtype=jnp.int32)
    indices = jnp.arange(NG, dtype=jnp.int32)
    cos_depth, sin_depth = tables(NZ, depth, bins)
    alternate = (1 - 2 * (depth % 2)).astype(jnp.float32)
    sin_packed = jnp.where(bins[None, :] == 0, -alternate[:, None], sin_depth)
    spec_re = jnp.einsum("xyz,zk->kxy", charges, cos_depth, precision=highest)
    spec_im = -jnp.einsum("xyz,zk->kxy", charges, sin_packed, precision=highest)
    own = jnp.moveaxis(green[:, :, :half], 2, 0)
    mirror = jnp.concatenate(
        [green[:, :, half : half + 1], jnp.flip(green[:, :, half + 1 :], 2)], axis=2
    )
    mirror = jnp.moveaxis(mirror, 2, 0)
    own, mirror = (
        lax.all_to_all(own, ("gy", "gz"), split_axis=0, concat_axis=2, tiled=True),
        lax.all_to_all(mirror, ("gy", "gz"), split_axis=0, concat_axis=2, tiled=True),
    )
    own, mirror = (
        lax.all_gather(own, "rep", axis=1, tiled=True),
        lax.all_gather(mirror, "rep", axis=1, tiled=True),
    )
    plane_re, plane_im = (
        lax.all_to_all(spec_re, ("gy", "gz"), split_axis=0, concat_axis=1, tiled=True),
        lax.all_to_all(spec_im, ("gy", "gz"), split_axis=0, concat_axis=1, tiled=True),
    )
    plane_re = plane_re.reshape(per_device, gy_count, NG, col_block)
    plane_im = plane_im.reshape(per_device, gy_count, NG, col_block)
    cos_plain, sin_plain = tables(NG, indices, indices)
    wide_cos = cos_plain.reshape(NG, gy_count, col_block)
    wide_sin = sin_plain.reshape(NG, gy_count, col_block)

    def second_in(matrix, values):
        return jnp.einsum("kgc,bgxc->bxk", matrix, values, precision=highest)

    def first_in(matrix, values):
        return jnp.einsum("kx,bxj->bkj", matrix, values, precision=highest)

    inner_re = second_in(wide_cos, plane_re) + second_in(wide_sin, plane_im)
    inner_im = second_in(wide_cos, plane_im) - second_in(wide_sin, plane_re)
    freq_re = first_in(cos_plain, inner_re) + first_in(sin_plain, inner_im)
    freq_im = first_in(cos_plain, inner_im) - first_in(sin_plain, inner_re)
    slot = lax.axis_index("gy") * gz_count + lax.axis_index("gz")
    packed = ((slot == 0) & (jnp.arange(per_device) == 0))[:, None, None]
    plain_gain = 0.5 * (own + reflect(mirror))
    first_gain = jnp.where(packed, 0.5 * (own + reflect(own)), plain_gain)
    second_gain = jnp.where(packed, 0.5 * (mirror + reflect(mirror)), plain_gain)
    mean_gain = 0.5 * (first_gain + second_gain)
    odd_gain = 0.5 * (first_gain - second_gain)
    prod_re = freq_re * mean_gain + reflect(freq_re) * odd_gain
    prod_im = freq_im * mean_gain - reflect(freq_im) * odd_gain
    undo_re = first_in(cos_plain, prod_re) - first_in(sin_plain, prod_im)
    undo_im = first_in(sin_plain, prod_re) + first_in(cos_plain, prod_im)

    def second_out(matrix, values):
        return jnp.einsum("kgc,bxk->bgxc", matrix, values, precision=highest)

    cells_re = second_out(wide_cos, undo_re) - second_out(wide_sin, undo_im)
    cells_im = second_out(wide_sin, undo_re) + second_out(wide_cos, undo_im)
    cells_re = cells_re.reshape(per_device, gy_count * NG, col_block)
    cells_im = cells_im.reshape(per_device, gy_count * NG, col_block)
    home_re, home_im = (
        lax.all_to_all(cells_re, ("gy", "gz"), split_axis=1, concat_axis=0, tiled=True),
        lax.all_to_all(cells_im, ("gy", "gz"), split_axis=1, concat_axis=0, tiled=True),
    )
    weight = jnp.where(bins == 0, 1.0, 2.0).astype(jnp.float32)
    cos_back = (cos_depth * weight[None, :]).T
    sin_back = jnp.where(bins[:, None] == 0, alternate[None, :], -2.0 * sin_depth.T)
    result_field = jnp.einsum("kxy,kz->xyz", home_re, cos_back, precision=highest)
    result_field = result_field + jnp.einsum("kxy,kz->xyz", home_im, sin_back, precision=highest)
    return result_field / (NG * NG * NZ)


f32 = jnp.float32
bf16 = jnp.bfloat16
MESH = pl.DeviceIdType.MESH
PARTS = 2


def split(values):
    high = values.astype(bf16)
    return high, (values - high.astype(f32)).astype(bf16)


def split_table(table):
    rounded = table.astype(jnp.bfloat16)
    high = jnp.asarray(rounded)
    low = jnp.asarray((table - rounded.astype(np.float64)).astype(jnp.bfloat16))
    return high, low


def dot(left, right, dims=((1,), (0,))):
    return lax.dot_general(left, right, (dims, ((), ())), preferred_element_type=f32)


def dot_table(values, table_high, table_low, dims=((1,), (0,))):
    high, low = split(values)
    return dot(high, table_high, dims) + (dot(low, table_high, dims) + dot(high, table_low, dims))


def table_dot(table_high, table_low, values, dims=((1,), (0,))):
    high, low = split(values)
    return dot(table_high, high, dims) + (dot(table_high, low, dims) + dot(table_low, high, dims))


def depth_tables(length, groups, bins_each):
    per_part = bins_each // PARTS
    forward, back = [], []
    z = np.arange(length)
    alternate = 1.0 - 2.0 * (z % 2)
    for start in range(0, groups * bins_each, per_part):
        for imaginary in (False, True):
            for k in range(start, start + per_part):
                angle = 2.0 * np.pi * ((k * z) % length) / length
                if k == 0:
                    forward.append(alternate if imaginary else np.ones(length))
                    back.append(alternate if imaginary else np.ones(length))
                else:
                    forward.append(-np.sin(angle) if imaginary else np.cos(angle))
                    back.append(-2.0 * np.sin(angle) if imaginary else 2.0 * np.cos(angle))
    return np.stack(forward), np.stack(back)


def depth_in_kernel(high_ref, low_ref, cells_ref, out_ref):
    rows, cols, depth = cells_ref.shape
    groups, parts, _, _ = out_ref.shape
    values = cells_ref[...].reshape(rows * cols, depth)
    result = table_dot(high_ref[...], low_ref[...], values, ((1,), (1,)))
    for row in range(rows):
        piece = result[:, row * cols : (row + 1) * cols]
        out_ref[:, :, row * 8 : (row + 1) * 8, :] = piece.reshape(groups, parts, 8, cols)


def depth_out_kernel(high_ref, low_ref, spec_ref, out_ref):
    rows, cols, depth = out_ref.shape
    pieces = [
        spec_ref[:, :, row * 8 : (row + 1) * 8, :].reshape(high_ref.shape[0], cols) for row in range(rows)
    ]
    values = jnp.concatenate(pieces, axis=1)
    result = dot_table(values, high_ref[...], low_ref[...], ((0,), (0,)))
    out_ref[...] = result.reshape(rows, cols, depth)


def pick_kernel(pick_ref, green_ref, out_ref):
    groups, parts, _, _ = out_ref.shape
    count = green_ref.shape[0] // 64
    rest = jnp.concatenate([green_ref[pl.ds(k2, 64, stride=count), :] for k2 in range(count)], axis=0)
    result = None
    for _ in range(3):
        high = rest.astype(bf16)
        rest = rest - high.astype(f32)
        term = dot(pick_ref[...], high, ((1,), (1,)))
        result = term if result is None else result + term
    size = groups * parts * 8
    first_lanes = lax.broadcasted_iota(jnp.int32, (size, 128), 1) < 64
    first_rows = lax.rem(lax.broadcasted_iota(jnp.int32, (size, 128), 0), 8) < 4
    for pair in range(count // 2):
        own = result[:size, pair * 128 : (pair + 1) * 128]
        mirror = result[size:, pair * 128 : (pair + 1) * 128]
        even = jnp.where(first_lanes, own, pltpu.roll(mirror, 64, 1))
        odd = jnp.where(first_lanes, pltpu.roll(own, 64, 1), mirror)
        out_ref[:, :, pair * 8 : (pair + 1) * 8, :] = jnp.where(first_rows, even, odd).reshape(groups, parts, 8, 128)


def planes_kernel(
    gy_count, gz_count, reps,
    spec_ref, gains_ref, waves_ref, flips_ref, home_ref,
    planes, green, freq, tables, flips,
    fwd_send, fwd_recv, back_send, back_recv, green_send, green_recv, right_send, left_send, line_recv, own_sem, table_sem,
):
    groups = gy_count * gz_count
    rep, gy, gz = lax.axis_index("rep"), lax.axis_index("gy"), lax.axis_index("gz")
    slot = gy * gz_count + gz
    rows = spec_ref.shape[2] // 8
    ng = flips_ref.shape[1]
    piece = gains_ref.shape[2]

    def partner(step):
        there_y = lax.rem(gy + step // gz_count, gy_count)
        there_z = lax.rem(gz + step % gz_count, gz_count)
        return there_y * gz_count + there_z, {"rep": rep, "gy": there_y, "gz": there_z}

    def along(step):
        return {"rep": lax.rem(rep + step + reps, reps), "gy": gy, "gz": gz}

    loads = []
    for table, (kind, swap) in enumerate(((1, False), (0, True), (0, False), (2, True))):
        minus, plus = (1, 2) if swap else (2, 1)
        for quadrant, wave in enumerate((0, minus, plus, 0)):
            loads.append(pltpu.make_async_copy(
                waves_ref.at[3 * kind + wave],
                tables.at[table, :, pl.ds(quadrant // 2 * ng, ng), pl.ds(quadrant % 2 * ng, ng)],
                table_sem.at[4 * table + quadrant]))
    loads.append(pltpu.make_async_copy(flips_ref, flips, table_sem.at[16]))
    for load in loads:
        load.start()

    order = sorted(range(1, groups), key=lambda s: (-(s % gz_count), s))

    barrier = pltpu.get_barrier_semaphore()
    for step in order:
        pl.semaphore_signal(barrier, inc=1, device_id=partner(step)[1], device_id_type=MESH)
    for step in (1, -1):
        pl.semaphore_signal(barrier, inc=1, device_id=along(step), device_id_type=MESH)
    pl.semaphore_wait(barrier, groups + 1)

    def green_copy(step, source, part):
        there, device = partner(step)
        return pltpu.make_async_remote_copy(
            src_ref=gains_ref.at[there, part], dst_ref=green.at[rep, part, pl.ds(source * piece, piece), :],
            send_sem=green_send.at[there, part], recv_sem=green_recv.at[source, part], device_id=device, device_id_type=MESH)

    def fwd_copy(step, source, part):
        there, device = partner(step)
        return pltpu.make_async_remote_copy(
            src_ref=spec_ref.at[there, part], dst_ref=planes.at[source, part],
            send_sem=fwd_send.at[there, part], recv_sem=fwd_recv.at[source, part], device_id=device, device_id_type=MESH)

    def back_copy(step, source, part):
        there, device = partner(step)
        return pltpu.make_async_remote_copy(
            src_ref=planes.at[there, part], dst_ref=home_ref.at[source, part],
            send_sem=back_send.at[there, part], recv_sem=back_recv.at[source, part], device_id=device, device_id_type=MESH)

    def line_copy(block, part, sem, step):
        return pltpu.make_async_remote_copy(
            src_ref=green.at[block, part], dst_ref=green.at[block, part], send_sem=sem.at[part],
            recv_sem=line_recv.at[block, part], device_id=along(step), device_id_type=MESH)

    own_green = [
        pltpu.make_async_copy(
            gains_ref.at[slot, h], green.at[rep, h, pl.ds(slot * piece, piece), :], own_sem.at[PARTS + h])
        for h in range(PARTS)
    ]
    own_planes = [pltpu.make_async_copy(spec_ref.at[slot, h], planes.at[slot, h], own_sem.at[h]) for h in range(PARTS)]
    for part in range(PARTS):
        for step in order:
            green_copy(step, slot, part).start()
    for copy in own_green + own_planes:
        copy.start()

    def line_start(part):
        @pl.when(rep + 1 < reps)
        def _():
            line_copy(rep, part, right_send.at[0], 1).start()

        @pl.when(rep >= 1)
        def _():
            line_copy(rep, part, left_send.at[0], -1).start()

    def relay(hop, part):
        @pl.when(rep >= hop)
        def _():
            line_copy(rep - hop, part, right_send.at[hop], 1).wait_recv()

        @pl.when((rep >= hop) & (rep + 1 < reps))
        def _():
            line_copy(rep - hop, part, right_send.at[hop], 1).start()

        @pl.when(rep + hop < reps)
        def _():
            line_copy(rep + hop, part, left_send.at[hop], -1).wait_recv()

        @pl.when((rep + hop < reps) & (rep >= 1))
        def _():
            line_copy(rep + hop, part, left_send.at[hop], -1).start()

    def load_plane(part, row):
        bands = []
        for y in range(gy_count):
            bands.append(jnp.concatenate(
                [planes[y * gz_count + x, part, pl.ds(row, rows, stride=8), :] for x in range(gz_count)], axis=0))
        return jnp.concatenate(bands, axis=1)

    def forward(part):
        def body(p, carry):
            values = jnp.concatenate([load_plane(part, p), load_plane(part, 4 + p)], axis=1)
            inner = dot_table(values, tables[0, 0], tables[0, 1])
            inner = jnp.concatenate([inner[:, :ng], inner[:, ng:]], axis=0)
            freq[part * 4 + p] = table_dot(tables[1, 0], tables[1, 1], inner)
            return carry

        lax.fori_loop(0, 4, body, 0)

    def reflect_plane(values):
        high, low = split(values)
        turned = dot(flips[0], high) + dot(flips[0], low)
        high, low = split(turned)
        return dot(high, flips[1]) + dot(low, flips[1])

    def backward(part):
        def body(p, carry):
            plane = part * 4 + p
            own, mirror = [], []
            lane = lax.broadcasted_iota(jnp.int32, (ng, 128), 1)
            for r in range(0, reps, 2):
                one, two = (
                    jnp.concatenate([green[q, part, pl.ds(4 * odd + p, ng // 2, stride=8), :] for odd in range(2)], axis=0)
                    for q in (r, r + 1)
                )
                own.append(jnp.where(lane < 64, one, pltpu.roll(two, 64, 1)))
                mirror.append(jnp.where(lane < 64, pltpu.roll(one, 64, 1), two))
            own = jnp.concatenate(own, axis=1).T
            mirror = jnp.concatenate(mirror, axis=1).T
            packed = (slot == 0) & (plane == 0)

            @pl.when(jnp.logical_not(packed))
            def _():
                gain = 0.5 * (own + reflect_plane(mirror))
                freq[plane] = freq[plane] * jnp.concatenate([gain, gain], axis=0)

            @pl.when(packed)
            def _():
                first = 0.5 * (own + reflect_plane(own))
                second = 0.5 * (mirror + reflect_plane(mirror))
                mean, odd = 0.5 * (first + second), 0.5 * (first - second)
                real, imag = freq[plane, :ng, :], freq[plane, ng:, :]
                freq[plane, :ng, :] = real * mean + reflect_plane(real) * odd
                freq[plane, ng:, :] = imag * mean - reflect_plane(imag) * odd

            undo = table_dot(tables[2, 0], tables[2, 1], freq[plane])
            undo = jnp.concatenate([undo[:ng], undo[ng:]], axis=1)
            cells = dot_table(undo, tables[3, 0], tables[3, 1])
            cols = ng // gy_count
            for c in range(2):
                for y in range(gy_count):
                    for x in range(gz_count):
                        planes[y * gz_count + x, part, pl.ds(c * 4 + p, rows, stride=8), :] = cells[
                            x * rows : (x + 1) * rows, c * ng + y * cols : c * ng + (y + 1) * cols]
            return carry

        lax.fori_loop(0, 4, body, 0)

    own_home = [pltpu.make_async_copy(planes.at[slot, h], home_ref.at[slot, h], own_sem.at[h]) for h in range(PARTS)]

    def arrive(part):
        own_planes[part].wait()
        for step in order:
            fwd_copy(step, partner(step)[0], part).wait_recv()
        forward(part)

    def depart(part):
        backward(part)
        for step in order:
            back_copy(step, slot, part).start()
        own_home[part].start()

    for part in range(PARTS):
        own_green[part].wait()
        for step in order:
            green_copy(step, partner(step)[0], part).wait_recv()
        if part == 0:
            line_start(0)
    for part in range(PARTS):
        for step in order:
            fwd_copy(step, slot, part).start()
    for hop in range(1, reps):
        relay(hop, 0)
    line_start(1)
    for load in loads:
        load.wait()
    arrive(0)
    depart(0)
    relay(1, 1)
    arrive(1)
    for hop in range(2, reps):
        relay(hop, 1)
    depart(1)

    for part in range(PARTS):
        for step in order:
            green_copy(step, slot, part).wait_send()
            fwd_copy(step, slot, part).wait_send()
        for hop in range(reps):
            @pl.when((rep >= hop) & (rep + 1 < reps))
            def _():
                line_copy(rep - hop, part, right_send.at[hop], 1).wait_send()

            @pl.when((rep + hop < reps) & (rep >= 1))
            def _():
                line_copy(rep + hop, part, left_send.at[hop], -1).wait_send()
    for part in range(PARTS):
        own_home[part].wait()
        for step in order:
            back_copy(step, slot, part).wait_send()
            back_copy(step, partner(step)[0], part).wait_recv()


def fused_plan(charges, green):
    gy_count, gz_count, reps = lax.axis_size("gy"), lax.axis_size("gz"), lax.axis_size("rep")
    groups = gy_count * gz_count
    rows, cols, depth = charges.shape
    ng = rows * gz_count
    half = depth // 2
    each = half // groups
    step = 8
    forward_table, back_table = depth_tables(depth, groups, each)
    fwd_h, fwd_l = split_table(forward_table)
    back_h, back_l = split_table(back_table / (ng * ng * depth))
    vmem = pl.BlockSpec(memory_space=pltpu.VMEM)
    table_spec = pl.BlockSpec((depth, depth), lambda i: (0, 0))
    cells_spec = pl.BlockSpec((step, cols, depth), lambda i: (i, 0, 0))
    spec_spec = pl.BlockSpec((groups, PARTS, step * 8, cols), lambda i: (0, 0, i, 0))
    spec_shape = jax.ShapeDtypeStruct((groups, PARTS, rows * 8, cols), f32)
    limit = pltpu.CompilerParams(vmem_limit_bytes=40 * 2**20)
    spec = pl.pallas_call(
        depth_in_kernel, grid=(rows // step,), out_shape=spec_shape, name="depth_in",
        in_specs=[table_spec, table_spec, cells_spec], out_specs=spec_spec, compiler_params=limit,
    )(fwd_h, fwd_l, charges)

    k1, k2, _ = green.shape
    own_index = np.arange(half)
    opposite = np.where(own_index == 0, half, depth - own_index)
    quads = np.repeat(np.arange(half // 4), 8) * 4 + np.tile(np.arange(4), half // 2)
    pick = np.zeros((2 * depth, depth), np.float32)
    pick[np.arange(depth), own_index[quads]] = 1.0
    pick[depth + np.arange(depth), opposite[quads]] = 1.0
    gains = pl.pallas_call(
        pick_kernel, out_shape=jax.ShapeDtypeStruct((groups, PARTS, k2 * 4, 2 * k1), f32), name="pick",
        in_specs=[vmem, vmem], out_specs=vmem, compiler_params=limit,
    )(jnp.asarray(pick, bf16), green.reshape(k1 * k2, depth))

    index = np.arange(ng)
    halves = np.concatenate([index[0::2], index[1::2]])
    angle = 2.0 * np.pi * ((index[:, None] * index[None, :]) % ng) / ng
    cos, sin = np.cos(angle), np.sin(angle)
    waves = np.stack([cos, sin, -sin])
    waves = np.concatenate([waves, waves[:, :, halves], waves[:, halves, :]])
    rounded = waves.astype(jnp.bfloat16)
    waves = jnp.asarray(np.stack([rounded, (waves - rounded.astype(np.float64)).astype(jnp.bfloat16)], axis=1))
    flips = np.stack([(rows_of[:, None] + rows_of[None, :]) % ng == 0 for rows_of in (index, halves)])
    flips = jnp.asarray(flips, bf16)

    dma = pltpu.SemaphoreType.DMA
    both = (groups, PARTS)
    home = pl.pallas_call(
        functools.partial(planes_kernel, gy_count, gz_count, reps),
        out_shape=spec_shape, name="planes",
        in_specs=[pl.BlockSpec(memory_space=pl.ANY)] * 4, out_specs=pl.BlockSpec(memory_space=pl.ANY),
        scratch_shapes=[
            pltpu.VMEM(spec_shape.shape, f32),
            pltpu.VMEM((reps, PARTS, ng * each // PARTS, 2 * k1), f32),
            pltpu.VMEM((each, 2 * ng, ng), f32),
            pltpu.VMEM((4, 2, 2 * ng, 2 * ng), bf16),
            pltpu.VMEM((2, ng, ng), bf16),
            dma(both), dma(both), dma(both), dma(both), dma(both), dma(both),
            dma((reps, PARTS)), dma((reps, PARTS)), dma((reps, PARTS)), dma((2 * PARTS,)), dma((17,)),
        ],
        compiler_params=pltpu.CompilerParams(
            collective_id=0, has_side_effects=True, vmem_limit_bytes=63 * 2**20),
    )(spec, gains, waves, flips)

    return pl.pallas_call(
        depth_out_kernel, grid=(rows // step,), out_shape=jax.ShapeDtypeStruct(charges.shape, f32), name="depth_out",
        in_specs=[table_spec, table_spec, spec_spec], out_specs=cells_spec, compiler_params=limit,
    )(back_h, back_l, home)


def on_device(charges, green):
    groups = lax.axis_size("gy") * lax.axis_size("gz")
    rows, cols, depth = charges.shape
    aligned = (
        cols % 128 == 0 and depth % 128 == 0 and depth == 16 * groups and rows % 8 == 0
        and green.shape[0] == 64 and lax.axis_size("rep") % 2 == 0 and lax.axis_size("rep") > 2
        and rows * lax.axis_size("gz") == cols * lax.axis_size("gy")
    )
    return fused_plan(charges, green) if aligned else slab_plan(charges, green)


def solution(mesh):
    placed = (P(("rep", "gz"), "gy", None), P("rep", ("gy", "gz"), None))
    return jax.shard_map(
        on_device,
        mesh=mesh,
        in_specs=placed,
        out_specs=P(("rep", "gz"), "gy", None),
        check_vma=False,
    )
```

```python
import functools
import math

import jax
import jax.numpy as jnp
import numpy as np
from jax import lax
from jax.experimental import pallas as pl
from jax.experimental.pallas import tpu as pltpu
from jax.sharding import PartitionSpec as P

NG = 256
NZ = 128


two_pi = 2.0 * math.pi
highest = lax.Precision.HIGHEST


def tables(length, rows_index, cols_index):
    phase = rows_index[:, None] * cols_index[None, :] % length
    angle = phase.astype(jnp.float32) * (two_pi / length)
    return (jnp.cos(angle), jnp.sin(angle))


def reflect(values):
    return jnp.roll(jnp.flip(values, (1, 2)), (1, 1), axis=(1, 2))


def slab_plan(charges, green):
    gy_count = lax.axis_size("gy")
    gz_count = lax.axis_size("gz")
    groups = gy_count * gz_count
    half = NZ // 2
    per_device = half // groups
    col_block = charges.shape[1]
    depth = jnp.arange(NZ, dtype=jnp.int32)
    bins = jnp.arange(half, dtype=jnp.int32)
    indices = jnp.arange(NG, dtype=jnp.int32)
    cos_depth, sin_depth = tables(NZ, depth, bins)
    alternate = (1 - 2 * (depth % 2)).astype(jnp.float32)
    sin_packed = jnp.where(bins[None, :] == 0, -alternate[:, None], sin_depth)
    spec_re = jnp.einsum("xyz,zk->kxy", charges, cos_depth, precision=highest)
    spec_im = -jnp.einsum("xyz,zk->kxy", charges, sin_packed, precision=highest)
    own = jnp.moveaxis(green[:, :, :half], 2, 0)
    mirror = jnp.concatenate(
        [green[:, :, half : half + 1], jnp.flip(green[:, :, half + 1 :], 2)], axis=2
    )
    mirror = jnp.moveaxis(mirror, 2, 0)
    own, mirror = (
        lax.all_to_all(own, ("gy", "gz"), split_axis=0, concat_axis=2, tiled=True),
        lax.all_to_all(mirror, ("gy", "gz"), split_axis=0, concat_axis=2, tiled=True),
    )
    own, mirror = (
        lax.all_gather(own, "rep", axis=1, tiled=True),
        lax.all_gather(mirror, "rep", axis=1, tiled=True),
    )
    plane_re, plane_im = (
        lax.all_to_all(spec_re, ("gy", "gz"), split_axis=0, concat_axis=1, tiled=True),
        lax.all_to_all(spec_im, ("gy", "gz"), split_axis=0, concat_axis=1, tiled=True),
    )
    plane_re = plane_re.reshape(per_device, gy_count, NG, col_block)
    plane_im = plane_im.reshape(per_device, gy_count, NG, col_block)
    cos_plain, sin_plain = tables(NG, indices, indices)
    wide_cos = cos_plain.reshape(NG, gy_count, col_block)
    wide_sin = sin_plain.reshape(NG, gy_count, col_block)

    def second_in(matrix, values):
        return jnp.einsum("kgc,bgxc->bxk", matrix, values, precision=highest)

    def first_in(matrix, values):
        return jnp.einsum("kx,bxj->bkj", matrix, values, precision=highest)

    inner_re = second_in(wide_cos, plane_re) + second_in(wide_sin, plane_im)
    inner_im = second_in(wide_cos, plane_im) - second_in(wide_sin, plane_re)
    freq_re = first_in(cos_plain, inner_re) + first_in(sin_plain, inner_im)
    freq_im = first_in(cos_plain, inner_im) - first_in(sin_plain, inner_re)
    slot = lax.axis_index("gy") * gz_count + lax.axis_index("gz")
    packed = ((slot == 0) & (jnp.arange(per_device) == 0))[:, None, None]
    plain_gain = 0.5 * (own + reflect(mirror))
    first_gain = jnp.where(packed, 0.5 * (own + reflect(own)), plain_gain)
    second_gain = jnp.where(packed, 0.5 * (mirror + reflect(mirror)), plain_gain)
    mean_gain = 0.5 * (first_gain + second_gain)
    odd_gain = 0.5 * (first_gain - second_gain)
    prod_re = freq_re * mean_gain + reflect(freq_re) * odd_gain
    prod_im = freq_im * mean_gain - reflect(freq_im) * odd_gain
    undo_re = first_in(cos_plain, prod_re) - first_in(sin_plain, prod_im)
    undo_im = first_in(sin_plain, prod_re) + first_in(cos_plain, prod_im)

    def second_out(matrix, values):
        return jnp.einsum("kgc,bxk->bgxc", matrix, values, precision=highest)

    cells_re = second_out(wide_cos, undo_re) - second_out(wide_sin, undo_im)
    cells_im = second_out(wide_sin, undo_re) + second_out(wide_cos, undo_im)
    cells_re = cells_re.reshape(per_device, gy_count * NG, col_block)
    cells_im = cells_im.reshape(per_device, gy_count * NG, col_block)
    home_re, home_im = (
        lax.all_to_all(cells_re, ("gy", "gz"), split_axis=1, concat_axis=0, tiled=True),
        lax.all_to_all(cells_im, ("gy", "gz"), split_axis=1, concat_axis=0, tiled=True),
    )
    weight = jnp.where(bins == 0, 1.0, 2.0).astype(jnp.float32)
    cos_back = (cos_depth * weight[None, :]).T
    sin_back = jnp.where(bins[:, None] == 0, alternate[None, :], -2.0 * sin_depth.T)
    result_field = jnp.einsum("kxy,kz->xyz", home_re, cos_back, precision=highest)
    result_field = result_field + jnp.einsum("kxy,kz->xyz", home_im, sin_back, precision=highest)
    return result_field / (NG * NG * NZ)


f32 = jnp.float32
bf16 = jnp.bfloat16
MESH = pl.DeviceIdType.MESH
PARTS = 2


def split(values):
    high = values.astype(bf16)
    return high, (values - high.astype(f32)).astype(bf16)


def stacked_table(table, axis):
    rounded = table.astype(jnp.bfloat16)
    return jnp.asarray(np.stack([rounded, (table - rounded.astype(np.float64)).astype(jnp.bfloat16)], axis=axis))


def split_table(table):
    rounded = table.astype(jnp.bfloat16)
    high = jnp.asarray(rounded)
    low = jnp.asarray((table - rounded.astype(np.float64)).astype(jnp.bfloat16))
    return high, low


def dot(left, right, dims=((1,), (0,))):
    return lax.dot_general(left, right, (dims, ((), ())), preferred_element_type=f32)


def dot_table(values, table_high, table_low, dims=((1,), (0,))):
    high, low = split(values)
    return dot(high, table_high, dims) + (dot(low, table_high, dims) + dot(high, table_low, dims))


def table_dot(table_high, table_low, values, dims=((1,), (0,))):
    high, low = split(values)
    return dot(table_high, high, dims) + (dot(table_high, low, dims) + dot(table_low, high, dims))


def depth_tables(length, groups, bins_each):
    per_part = bins_each // PARTS
    forward, back = [], []
    z = np.arange(length)
    alternate = 1.0 - 2.0 * (z % 2)
    for start in range(0, groups * bins_each, per_part):
        for imaginary in (False, True):
            for k in range(start, start + per_part):
                angle = 2.0 * np.pi * ((k * z) % length) / length
                if k == 0:
                    forward.append(alternate if imaginary else np.ones(length))
                    back.append(alternate if imaginary else np.ones(length))
                else:
                    forward.append(-np.sin(angle) if imaginary else np.cos(angle))
                    back.append(-2.0 * np.sin(angle) if imaginary else 2.0 * np.cos(angle))
    return np.stack(forward), np.stack(back)


def depth_in(table, cells, out):
    groups, parts, _, cols = out.shape
    rows, depth, step = cells.shape[0], cells.shape[2], 8

    def body(i, carry):
        values = cells[pl.ds(i * step, step)].reshape(step * cols, depth)
        result = table_dot(table[0], table[1], values, ((1,), (1,)))
        for row in range(step):
            piece = result[:, row * cols : (row + 1) * cols]
            at = pl.multiple_of(i * (step * 8) + row * 8, 8)
            out[:, :, pl.ds(at, 8), :] = piece.reshape(groups, parts, 8, cols)
        return carry

    lax.fori_loop(0, rows // step, body, 0)


def depth_out_kernel(high_ref, low_ref, spec_ref, out_ref):
    rows, cols, depth = out_ref.shape
    pieces = [
        spec_ref[:, :, row * 8 : (row + 1) * 8, :].reshape(high_ref.shape[0], cols) for row in range(rows)
    ]
    values = jnp.concatenate(pieces, axis=1)
    result = dot_table(values, high_ref[...], low_ref[...], ((0,), (0,)))
    out_ref[...] = result.reshape(rows, cols, depth)


def pick_green(pick_ref, green_ref, out_ref):
    groups, parts, _, _ = out_ref.shape
    count = green_ref.shape[0] // 64
    rest = jnp.concatenate([green_ref[pl.ds(k2, 64, stride=count), :] for k2 in range(count)], axis=0)
    result = None
    for _ in range(3):
        high = rest.astype(bf16)
        rest = rest - high.astype(f32)
        term = dot(pick_ref[...], high, ((1,), (1,)))
        result = term if result is None else result + term
    size = groups * parts * 8
    first_lanes = lax.broadcasted_iota(jnp.int32, (size, 128), 1) < 64
    first_rows = lax.rem(lax.broadcasted_iota(jnp.int32, (size, 128), 0), 8) < 4
    for pair in range(count // 2):
        own = result[:size, pair * 128 : (pair + 1) * 128]
        mirror = result[size:, pair * 128 : (pair + 1) * 128]
        even = jnp.where(first_lanes, own, pltpu.roll(mirror, 64, 1))
        odd = jnp.where(first_lanes, pltpu.roll(own, 64, 1), mirror)
        out_ref[:, :, pair * 8 : (pair + 1) * 8, :] = jnp.where(first_rows, even, odd).reshape(groups, parts, 8, 128)


def planes_kernel(
    gy_count, gz_count, reps,
    cells_in, green_in, pick_in, depth_table, waves_ref, flips_ref, home_ref,
    cells_ref, field_ref, pick_ref, depth_ref, gains_ref, spec_ref,
    planes, green, freq, tables, flips,
    fwd_send, fwd_recv, back_send, back_recv, green_send, green_recv, right_send, left_send, line_recv, own_sem, table_sem, in_sem,
):
    groups = gy_count * gz_count
    rep, gy, gz = lax.axis_index("rep"), lax.axis_index("gy"), lax.axis_index("gz")
    slot = gy * gz_count + gz
    rows = spec_ref.shape[2] // 8
    ng = flips_ref.shape[1]
    piece = gains_ref.shape[2]

    def partner(step):
        there_y = lax.rem(gy + step // gz_count, gy_count)
        there_z = lax.rem(gz + step % gz_count, gz_count)
        return there_y * gz_count + there_z, {"rep": rep, "gy": there_y, "gz": there_z}

    def along(step):
        return {"rep": lax.rem(rep + step + reps, reps), "gy": gy, "gz": gz}

    inputs = [
        pltpu.make_async_copy(source, held, in_sem.at[i])
        for i, (source, held) in enumerate((
            (green_in, field_ref), (pick_in, pick_ref), (cells_in, cells_ref), (depth_table, depth_ref)))
    ]
    for copy in inputs:
        copy.start()

    loads = []
    for table, (kind, swap) in enumerate(((1, False), (0, True), (0, False), (2, True))):
        minus, plus = (1, 2) if swap else (2, 1)
        for quadrant, wave in enumerate((0, minus, plus, 0)):
            loads.append(pltpu.make_async_copy(
                waves_ref.at[3 * kind + wave],
                tables.at[table, :, pl.ds(quadrant // 2 * ng, ng), pl.ds(quadrant % 2 * ng, ng)],
                table_sem.at[4 * table + quadrant]))
    loads.append(pltpu.make_async_copy(flips_ref, flips, table_sem.at[16]))
    for load in loads:
        load.start()

    order = sorted(range(1, groups), key=lambda s: (-(s % gz_count), s))

    barrier = pltpu.get_barrier_semaphore()
    for step in order:
        pl.semaphore_signal(barrier, inc=1, device_id=partner(step)[1], device_id_type=MESH)
    for step in (1, -1):
        pl.semaphore_signal(barrier, inc=1, device_id=along(step), device_id_type=MESH)
    for copy in inputs[:2]:
        copy.wait()
    pick_green(pick_ref, field_ref, gains_ref)
    pl.semaphore_wait(barrier, groups + 1)

    def green_copy(step, source, part):
        there, device = partner(step)
        return pltpu.make_async_remote_copy(
            src_ref=gains_ref.at[there, part], dst_ref=green.at[rep, part, pl.ds(source * piece, piece), :],
            send_sem=green_send.at[there, part], recv_sem=green_recv.at[source, part], device_id=device, device_id_type=MESH)

    def fwd_copy(step, source, part):
        there, device = partner(step)
        return pltpu.make_async_remote_copy(
            src_ref=spec_ref.at[there, part], dst_ref=planes.at[source, part],
            send_sem=fwd_send.at[there, part], recv_sem=fwd_recv.at[source, part], device_id=device, device_id_type=MESH)

    def back_copy(step, source, part):
        there, device = partner(step)
        return pltpu.make_async_remote_copy(
            src_ref=planes.at[there, part], dst_ref=home_ref.at[source, part],
            send_sem=back_send.at[there, part], recv_sem=back_recv.at[source, part], device_id=device, device_id_type=MESH)

    def line_copy(block, part, sem, step):
        return pltpu.make_async_remote_copy(
            src_ref=green.at[block, part], dst_ref=green.at[block, part], send_sem=sem.at[part],
            recv_sem=line_recv.at[block, part], device_id=along(step), device_id_type=MESH)

    own_green = [
        pltpu.make_async_copy(
            gains_ref.at[slot, h], green.at[rep, h, pl.ds(slot * piece, piece), :], own_sem.at[PARTS + h])
        for h in range(PARTS)
    ]
    own_planes = [pltpu.make_async_copy(spec_ref.at[slot, h], planes.at[slot, h], own_sem.at[h]) for h in range(PARTS)]
    for part in range(PARTS):
        for step in order:
            green_copy(step, slot, part).start()
    for copy in own_green:
        copy.start()
    for copy in inputs[2:]:
        copy.wait()
    depth_in(depth_ref, cells_ref, spec_ref)
    for copy in own_planes:
        copy.start()

    def line_start(part):
        @pl.when(rep + 1 < reps)
        def _():
            line_copy(rep, part, right_send.at[0], 1).start()

        @pl.when(rep >= 1)
        def _():
            line_copy(rep, part, left_send.at[0], -1).start()

    def relay(hop, part):
        @pl.when(rep >= hop)
        def _():
            line_copy(rep - hop, part, right_send.at[hop], 1).wait_recv()

        @pl.when((rep >= hop) & (rep + 1 < reps))
        def _():
            line_copy(rep - hop, part, right_send.at[hop], 1).start()

        @pl.when(rep + hop < reps)
        def _():
            line_copy(rep + hop, part, left_send.at[hop], -1).wait_recv()

        @pl.when((rep + hop < reps) & (rep >= 1))
        def _():
            line_copy(rep + hop, part, left_send.at[hop], -1).start()

    def load_plane(part, row):
        bands = []
        for y in range(gy_count):
            bands.append(jnp.concatenate(
                [planes[y * gz_count + x, part, pl.ds(row, rows, stride=8), :] for x in range(gz_count)], axis=0))
        return jnp.concatenate(bands, axis=1)

    def forward(part):
        def body(p, carry):
            values = jnp.concatenate([load_plane(part, p), load_plane(part, 4 + p)], axis=1)
            inner = dot_table(values, tables[0, 0], tables[0, 1])
            inner = jnp.concatenate([inner[:, :ng], inner[:, ng:]], axis=0)
            freq[part * 4 + p] = table_dot(tables[1, 0], tables[1, 1], inner)
            return carry

        lax.fori_loop(0, 4, body, 0)

    def reflect_plane(values):
        high, low = split(values)
        turned = dot(flips[0], high) + dot(flips[0], low)
        high, low = split(turned)
        return dot(high, flips[1]) + dot(low, flips[1])

    def backward(part):
        def body(p, carry):
            plane = part * 4 + p
            own, mirror = [], []
            lane = lax.broadcasted_iota(jnp.int32, (ng, 128), 1)
            for r in range(0, reps, 2):
                one, two = (
                    jnp.concatenate([green[q, part, pl.ds(4 * odd + p, ng // 2, stride=8), :] for odd in range(2)], axis=0)
                    for q in (r, r + 1)
                )
                own.append(jnp.where(lane < 64, one, pltpu.roll(two, 64, 1)))
                mirror.append(jnp.where(lane < 64, pltpu.roll(one, 64, 1), two))
            own = jnp.concatenate(own, axis=1).T
            mirror = jnp.concatenate(mirror, axis=1).T
            packed = (slot == 0) & (plane == 0)

            @pl.when(jnp.logical_not(packed))
            def _():
                gain = 0.5 * (own + reflect_plane(mirror))
                freq[plane] = freq[plane] * jnp.concatenate([gain, gain], axis=0)

            @pl.when(packed)
            def _():
                first = 0.5 * (own + reflect_plane(own))
                second = 0.5 * (mirror + reflect_plane(mirror))
                mean, odd = 0.5 * (first + second), 0.5 * (first - second)
                real, imag = freq[plane, :ng, :], freq[plane, ng:, :]
                freq[plane, :ng, :] = real * mean + reflect_plane(real) * odd
                freq[plane, ng:, :] = imag * mean - reflect_plane(imag) * odd

            undo = table_dot(tables[2, 0], tables[2, 1], freq[plane])
            undo = jnp.concatenate([undo[:ng], undo[ng:]], axis=1)
            cells = dot_table(undo, tables[3, 0], tables[3, 1])
            cols = ng // gy_count
            for c in range(2):
                for y in range(gy_count):
                    for x in range(gz_count):
                        planes[y * gz_count + x, part, pl.ds(c * 4 + p, rows, stride=8), :] = cells[
                            x * rows : (x + 1) * rows, c * ng + y * cols : c * ng + (y + 1) * cols]
            return carry

        lax.fori_loop(0, 4, body, 0)

    own_home = [pltpu.make_async_copy(planes.at[slot, h], home_ref.at[slot, h], own_sem.at[h]) for h in range(PARTS)]

    def arrive(part):
        own_planes[part].wait()
        for step in order:
            fwd_copy(step, partner(step)[0], part).wait_recv()
        forward(part)

    def depart(part):
        backward(part)
        for step in order:
            back_copy(step, slot, part).start()
        own_home[part].start()

    for part in range(PARTS):
        own_green[part].wait()
        for step in order:
            green_copy(step, partner(step)[0], part).wait_recv()
        if part == 0:
            line_start(0)
    for part in range(PARTS):
        for step in order:
            fwd_copy(step, slot, part).start()
    for hop in range(1, reps):
        relay(hop, 0)
    line_start(1)
    for load in loads:
        load.wait()
    arrive(0)
    depart(0)
    relay(1, 1)
    arrive(1)
    for hop in range(2, reps):
        relay(hop, 1)
    depart(1)

    for part in range(PARTS):
        for step in order:
            green_copy(step, slot, part).wait_send()
            fwd_copy(step, slot, part).wait_send()
        for hop in range(reps):
            @pl.when((rep >= hop) & (rep + 1 < reps))
            def _():
                line_copy(rep - hop, part, right_send.at[hop], 1).wait_send()

            @pl.when((rep + hop < reps) & (rep >= 1))
            def _():
                line_copy(rep + hop, part, left_send.at[hop], -1).wait_send()
    for part in range(PARTS):
        own_home[part].wait()
        for step in order:
            back_copy(step, slot, part).wait_send()
            back_copy(step, partner(step)[0], part).wait_recv()


def fused_plan(charges, green):
    gy_count, gz_count, reps = lax.axis_size("gy"), lax.axis_size("gz"), lax.axis_size("rep")
    groups = gy_count * gz_count
    rows, cols, depth = charges.shape
    ng = rows * gz_count
    half = depth // 2
    each = half // groups
    step = 8
    forward_table, back_table = depth_tables(depth, groups, each)
    back_h, back_l = split_table(back_table / (ng * ng * depth))
    table_spec = pl.BlockSpec((depth, depth), lambda i: (0, 0))
    cells_spec = pl.BlockSpec((step, cols, depth), lambda i: (i, 0, 0))
    spec_spec = pl.BlockSpec((groups, PARTS, step * 8, cols), lambda i: (0, 0, i, 0))
    spec_shape = jax.ShapeDtypeStruct((groups, PARTS, rows * 8, cols), f32)
    limit = pltpu.CompilerParams(vmem_limit_bytes=63 * 2**20)

    k1, k2, _ = green.shape
    own_index = np.arange(half)
    opposite = np.where(own_index == 0, half, depth - own_index)
    quads = np.repeat(np.arange(half // 4), 8) * 4 + np.tile(np.arange(4), half // 2)
    pick = np.zeros((2 * depth, depth), np.float32)
    pick[np.arange(depth), own_index[quads]] = 1.0
    pick[depth + np.arange(depth), opposite[quads]] = 1.0
    index = np.arange(ng)
    halves = np.concatenate([index[0::2], index[1::2]])
    angle = 2.0 * np.pi * ((index[:, None] * index[None, :]) % ng) / ng
    cos, sin = np.cos(angle), np.sin(angle)
    waves = np.stack([cos, sin, -sin])
    waves = np.concatenate([waves, waves[:, :, halves], waves[:, halves, :]])
    waves = stacked_table(waves, 1)
    flips = np.stack([(rows_of[:, None] + rows_of[None, :]) % ng == 0 for rows_of in (index, halves)])
    flips = jnp.asarray(flips, bf16)

    dma = pltpu.SemaphoreType.DMA
    both = (groups, PARTS)
    home = pl.pallas_call(
        functools.partial(planes_kernel, gy_count, gz_count, reps),
        out_shape=spec_shape, name="planes",
        in_specs=[pl.BlockSpec(memory_space=pl.ANY)] * 6, out_specs=pl.BlockSpec(memory_space=pl.ANY),
        scratch_shapes=[
            pltpu.VMEM(charges.shape, f32),
            pltpu.VMEM((k1 * k2, depth), f32),
            pltpu.VMEM(pick.shape, bf16),
            pltpu.VMEM((2, depth, depth), bf16),
            pltpu.VMEM((groups, PARTS, k2 * 4, 2 * k1), f32),
            pltpu.VMEM(spec_shape.shape, f32),
            pltpu.VMEM(spec_shape.shape, f32),
            pltpu.VMEM((reps, PARTS, ng * each // PARTS, 2 * k1), f32),
            pltpu.VMEM((each, 2 * ng, ng), f32),
            pltpu.VMEM((4, 2, 2 * ng, 2 * ng), bf16),
            pltpu.VMEM((2, ng, ng), bf16),
            dma(both), dma(both), dma(both), dma(both), dma(both), dma(both),
            dma((reps, PARTS)), dma((reps, PARTS)), dma((reps, PARTS)), dma((2 * PARTS,)), dma((17,)), dma((4,)),
        ],
        compiler_params=pltpu.CompilerParams(
            collective_id=0, has_side_effects=True, vmem_limit_bytes=63 * 2**20),
    )(charges, green.reshape(k1 * k2, depth), jnp.asarray(pick, bf16), stacked_table(forward_table, 0), waves, flips)

    return pl.pallas_call(
        depth_out_kernel, grid=(rows // step,), out_shape=jax.ShapeDtypeStruct(charges.shape, f32), name="depth_out",
        in_specs=[table_spec, table_spec, spec_spec], out_specs=cells_spec, compiler_params=limit,
    )(back_h, back_l, home)


def on_device(charges, green):
    groups = lax.axis_size("gy") * lax.axis_size("gz")
    rows, cols, depth = charges.shape
    aligned = (
        cols % 128 == 0 and depth % 128 == 0 and depth == 16 * groups and rows % 8 == 0
        and green.shape[0] == 64 and lax.axis_size("rep") % 2 == 0 and lax.axis_size("rep") > 2
        and rows * lax.axis_size("gz") == cols * lax.axis_size("gy")
    )
    return fused_plan(charges, green) if aligned else slab_plan(charges, green)


def solution(mesh):
    placed = (P(("rep", "gz"), "gy", None), P("rep", ("gy", "gz"), None))
    return jax.shard_map(
        on_device,
        mesh=mesh,
        in_specs=placed,
        out_specs=P(("rep", "gz"), "gy", None),
        check_vma=False,
    )
```
